32 devices in a mesh: fr: 2 (over core), sr: 4 (over z), sc: 4 (over y, x).
Axes of the slice: x: 2, y: 2, z: 4, core: 2. Of those that a mesh axis runs over, the one named last changes fastest.
Arguments:
- spec_re: bfloat16 [8, 2048, 256], P('fr', ('sr', 'sc')), may hold values from -6 to 6
- spec_im: bfloat16 [8, 2048, 256], P('fr', ('sr', 'sc')), may hold values from -6 to 6
- offsets: int32 [16, 9], P(('sr', 'sc')), may hold values from 0 to 8, each once within a row
Outputs:
- cross: float32 [8, 16, 9, 128, 256], P('fr', ('sr', 'sc'))
The draws below stay inside these ranges and needn't reach their ends.
Inputs may be any that keep to these rules, and one draw needn't show every extreme that they name: Each row of offsets names every offset 0 to 8 exactly once.
All inputs are finite; a program needn't handle non-finite values.
Results may differ from the reference program's by a relative error of at most 0.0003.
Values may be sent and summed in bfloat16 or wider, within the bound.
No kernel may reach another device: no remote copies, remote signals or barrier semaphores. Data moves between devices by JAX's collectives and lax.ppermute only.
A program may use at most 128 MiB of HBM per device.

```python
import math
import jax
import jax.numpy as jnp
from jax import lax

BLK = 128
SEG = 256
NB = 16
HALF = 9
STATIONS = 2048
FREQ = 8


def block_levels(stream_key, dims, split, low, top_value):
    gain = 1.0
    for position, blocks in split:
        draws = jax.random.uniform(jax.random.fold_in(jax.random.fold_in(stream_key, 6), position), (blocks,), jnp.float32, low / len(split), top_value / len(split))
        gain = gain * jnp.repeat(jnp.exp(draws), dims[position] // blocks).reshape((-1,) + (1,) * (len(dims) - 1 - position))
    return gain


def centred(key, shape, deviation, reach, cuts=(), held_as=jnp.bfloat16):
    values = jax.random.normal(key, shape, jnp.float32) * deviation
    if len(cuts) > 0:
        values = block_levels(key, shape, cuts, -0.22, 0.18) * values
    return jnp.clip(values, min=-reach, max=reach).astype(held_as)


def setup_inputs(seed: int = 0) -> dict:
    arg_keys = jax.random.split(jax.random.key(seed), 4)
    spec_re = centred(arg_keys[0], (FREQ, STATIONS, SEG), 1.0, 6.0, ((0, 2), (1, 16)))
    spec_im = centred(arg_keys[1], (FREQ, STATIONS, SEG), 1.0, 6.0, ((0, 2), (1, 16)))
    offsets = jax.vmap(lambda own: jax.random.permutation(own, HALF))(jax.random.split(arg_keys[2], NB)).reshape((NB, HALF)).astype(jnp.int32)
    return {"spec_re": spec_re, "spec_im": spec_im, "offsets": offsets}


def reference(spec_re, spec_im, offsets):
    real_full = spec_re.astype(jnp.float32)
    imag_full = spec_im.astype(jnp.float32)
    band_power = lax.optimization_barrier(jnp.sum(real_full * real_full + imag_full * imag_full, axis=(0, 2))) / (FREQ * SEG)
    gain_table = (1.0 / jnp.sqrt(band_power)).reshape(NB, BLK)
    real_blocks = real_full.reshape(FREQ, NB, BLK, SEG)
    imag_blocks = imag_full.reshape(FREQ, NB, BLK, SEG)
    norm_scale = 1.0 / math.sqrt(SEG)
    highest = lax.Precision.HIGHEST

    def one_block(block_index):
        partners = ((block_index + offsets[block_index]) % NB).astype(jnp.int32)
        own_re = real_blocks[:, block_index]
        own_im = imag_blocks[:, block_index]
        other_re = real_blocks[:, partners]
        other_im = imag_blocks[:, partners]
        real_part = jnp.einsum('fis,fmjs->fmij', own_re, other_re, precision=highest) + jnp.einsum('fis,fmjs->fmij', own_im, other_im, precision=highest)
        imag_part = jnp.einsum('fis,fmjs->fmij', own_im, other_re, precision=highest) - jnp.einsum('fis,fmjs->fmij', own_re, other_im, precision=highest)
        weight = gain_table[block_index][None, None, :, None] * gain_table[partners][None, :, None, :] * norm_scale
        return jnp.concatenate([real_part * weight, imag_part * weight], axis=-1)
    joined = lax.map(one_block, jnp.arange(NB, dtype=jnp.int32))
    return jnp.transpose(joined, (1, 0, 2, 3, 4))
```

```python
import functools
import math

import jax
import jax.numpy as jnp
from jax import lax
from jax.experimental import pallas as pl
from jax.experimental.pallas import tpu as pltpu
from jax.sharding import PartitionSpec as P


BLOCKS = ("sr", "sc")
GAIN_PARTS = 3
GAIN_ROWS = 16


def product_kernel(
    pair_count, norm, slot_ref, re_ref, im_ref, weight_ref, *refs
):
    reals = refs[:pair_count]
    imags = refs[pair_count : 2 * pair_count]
    out_ref, stage, sems = refs[-3:]
    bins, rows, segs = re_ref.shape
    contract = (((1,), (1,)), ((), ()))

    def copy_out(i, f):
        return pltpu.make_async_copy(
            stage.at[i, f], out_ref.at[f, 0, slot_ref[i]], sems.at[i, f]
        )

    for i in range(pair_count):

        @pl.when(slot_ref[i] >= 0)
        def _(i=i):
            parts = imags[i][pl.ds(bins * rows, GAIN_ROWS), :rows].astype(jnp.float32)
            gain = parts[0:1] + parts[1:2] + parts[2:3]
            weight = weight_ref[...] * gain

            for f in range(bins):
                own = jnp.concatenate([re_ref[f], im_ref[f]], axis=0)
                turned = jnp.concatenate([im_ref[f], -re_ref[f]], axis=0)
                other_re = reals[i][f]
                other_im = imags[i][pl.ds(f * rows, rows), :]
                first = lax.dot_general(
                    own, other_re, contract, preferred_element_type=jnp.float32
                )
                second = lax.dot_general(
                    turned, other_im, contract, preferred_element_type=jnp.float32
                )
                both = first + second
                stage[i, f, :, :rows] = both[:rows] * weight
                stage[i, f, :, rows:] = both[rows:] * weight
                copy_out(i, f).start()

    for i in range(pair_count):

        @pl.when(slot_ref[i] >= 0)
        def _(i=i):
            for f in range(bins):
                copy_out(i, f).wait()


def products(slots, re_own, im_own, weight, pairs, out_shape, out=None, name="p"):
    bins, rows, segs = re_own.shape
    count = len(pairs)
    vmem = pl.BlockSpec(memory_space=pltpu.VMEM)
    args = [slots, re_own, im_own, weight] + [a for a, _ in pairs] + [b for _, b in pairs]
    specs = [pl.BlockSpec(memory_space=pltpu.SMEM)] + [vmem] * (len(args) - 1)
    aliases = {}
    if out is not None:
        aliases = {len(args): 0}
        args.append(out)
        specs.append(pl.BlockSpec(memory_space=pl.ANY))
    body = functools.partial(product_kernel, count, 1.0)
    flops = count * bins * 4 * 2 * rows * rows * segs
    return pl.pallas_call(
        body,
        out_shape=out_shape,
        in_specs=specs,
        out_specs=pl.BlockSpec(memory_space=pl.ANY),
        scratch_shapes=[
            pltpu.VMEM((count, bins, rows, 2 * rows), jnp.float32),
            pltpu.SemaphoreType.DMA((count, bins)),
        ],
        input_output_aliases=aliases,
        cost_estimate=pl.CostEstimate(
            flops=flops, bytes_accessed=count * bins * rows * 2 * rows * 4, transcendentals=0
        ),
        name=name,
    )(*args)


def local(sr, sc, spec_re, spec_im, offsets):
    bins, rows, segs = spec_re.shape
    blocks = sr * sc
    slot_count = offsets.shape[1]
    half = sr // 2
    bin_total = bins * lax.axis_size("fr")
    column = lax.axis_index("sc")
    norm = 1.0 / math.sqrt(segs)

    def send(value, route):
        links = []
        for z in range(sr):
            for s in range(sc):
                target = route(z, s)
                if target is not None:
                    links.append((z * sc + s, (target[0] % sr) * sc + target[1]))
        return lax.ppermute(value, BLOCKS, links)

    def down(columns=range(sc)):
        return lambda z, s: (z - 1, s) if s in columns else None

    def flip(bit, columns=range(sc)):
        return lambda z, s: (z, s ^ bit) if s in columns else None

    re32 = spec_re.astype(jnp.float32)
    im32 = spec_im.astype(jnp.float32)
    power_half = jnp.sum(re32 * re32 + im32 * im32, axis=(0, 2))
    power = power_half + lax.ppermute(power_half, "fr", [(0, 1), (1, 0)])
    gain = lax.rsqrt(power / (bin_total * segs))
    parts, rest = [], gain
    for _ in range(GAIN_PARTS):
        part = lax.reduce_precision(rest, exponent_bits=8, mantissa_bits=7)
        parts.append(part)
        rest = rest - part
    tail = jnp.stack(parts).astype(jnp.bfloat16)
    tail = jnp.pad(tail, ((0, GAIN_ROWS - GAIN_PARTS), (0, segs - rows)))
    weight = jnp.broadcast_to((gain * norm)[:, None], (rows, rows))

    own_a = spec_re
    own_b = jnp.concatenate([spec_im.reshape(bins * rows, segs), tail], axis=0)

    def both(pair, route):
        return send(pair[0], route), send(pair[1], route)

    own = (own_a, own_b)
    upper = [s for s in range(sc) if s & 2]
    lower = [s for s in range(sc) if not s & 2]
    odd = [s for s in range(sc) if s & 1]

    jobs_1, jobs_2, jobs_3 = [], [], []
    everyone = range(sc)
    planes = [own]
    for j in range(half):
        planes.append(both(planes[-1], down()))
    near, far = planes[half - 1], planes[half]
    near_x = both(own, flip(1, odd)), both(near, flip(1))
    near_y = both(own, flip(2, upper)), both(near, flip(2))
    u1, u2 = near_x
    v1, v2 = near_y
    is_upper = (column & 2) != 0

    def pick(flag, yes, no):
        return jnp.where(flag, yes, no)

    x3 = tuple(send(pick(is_upper, v2[h], v1[h]), flip(1)) for h in range(2))
    y3 = tuple(send(pick(is_upper, u2[h], far[h]), flip(2)) for h in range(2))
    z3_b = send(u2[1], down([0, 1, 3]))
    z3_a = send(pick(column == 2, x3[0], u2[0]), down([1, 2, 3]))
    xf_a = send(y3[0], flip(1, [2]))
    yf_b = send(z3_b, flip(2, [0, 1]))

    def offset(plane, xor):
        return plane * sc + (column ^ xor) - column

    def slot(k, wanted=True):
        k = jnp.where(jnp.logical_and(wanted, jnp.logical_and(k >= 0, k < slot_count)), k, -1)
        hits = (offsets[0] == k).astype(jnp.int32)
        position = jnp.sum(hits * jnp.arange(slot_count, dtype=jnp.int32))
        return jnp.where(k >= 0, position, -1)

    groups = [
        [
            (own, slot(offset(0, 0))),
            (near, slot(offset(half - 1, 0))),
            (u1, slot(offset(0, 1))),
            (v1, slot(offset(0, 2))),
        ],
        [
            (u2, slot(offset(half - 1, 1))),
            (v2, slot(offset(half - 1, 2))),
            (far, slot(offset(half, 0))),
        ],
    ]
    for j in range(1, half - 1):
        u = both(planes[j], flip(1))
        v = both(planes[j], flip(2))
        d = both(v, flip(1))
        groups.append(
            [
                (planes[j], slot(offset(j, 0))),
                (u, slot(offset(j, 1))),
                (v, slot(offset(j, 2))),
                (d, slot(offset(j, 3))),
            ]
        )
    groups.append(
        [
            (x3, slot(jnp.where(is_upper, offset(half - 1, 3), offset(0, 3)))),
            (y3, slot(jnp.where(is_upper, offset(half, 2), offset(half - 1, 3)))),
            ((z3_a, z3_b), slot(offset(half, 1), (column & 1) == 1)),
            ((z3_a, yf_b), slot(offset(half, 3), column == 2)),
            ((xf_a, yf_b), slot(offset(half, 3), column == 3)),
        ]
    )
    out_shape = jax.ShapeDtypeStruct((bins, 1, slot_count, rows, 2 * rows), jnp.float32)
    out = None
    for n, group in enumerate(groups):
        slots = jnp.stack([s for _, s in group]).astype(jnp.int32)
        out = products(
            slots, spec_re, spec_im, weight, [p for p, _ in group], out_shape, out, f"prod{n}"
        )
    return out


def solution(mesh):
    placed = (P("fr", ("sr", "sc"), None), P("fr", ("sr", "sc"), None), P(("sr", "sc"), None))
    return jax.shard_map(
        functools.partial(local, mesh.shape["sr"], mesh.shape["sc"]),
        mesh=mesh,
        in_specs=placed,
        out_specs=P("fr", ("sr", "sc"), None, None, None),
        check_vma=False,
    )
```

```python
import functools
import math

import jax
import jax.numpy as jnp
from jax import lax
from jax.experimental import pallas as pl
from jax.experimental.pallas import tpu as pltpu
from jax.sharding import PartitionSpec as P


BLOCKS = ("sr", "sc")
GAIN_PARTS = 3
GAIN_ROWS = 16
VMEM_BYTES = 16 << 20


def product_kernel(entries, offsets_ref, re_ref, im_ref, weight_ref, *refs):
    pair_count = len(entries)
    reals = refs[:pair_count]
    imags = refs[pair_count : 2 * pair_count]
    out_ref, stage, sems = refs[-3:]
    bins, rows, _ = re_ref.shape
    slot_count = offsets_ref.shape[1]
    contract = (((1,), (1,)), ((), ()))
    column = lax.axis_index("sc")

    wanted, slots = [], []
    for entry in entries:
        offset, use = entry(column)
        use = jnp.logical_and(use, jnp.logical_and(offset >= 0, offset < slot_count))

        def find(m, found, offset=offset):
            return jnp.where(offsets_ref[0, m] == offset, m, found)

        wanted.append(use)
        slots.append(lax.fori_loop(0, slot_count, find, jnp.int32(0), unroll=True))

    def copy_out(i, f):
        return pltpu.make_async_copy(
            stage.at[i, f], out_ref.at[f, 0, slots[i]], sems.at[i, f]
        )

    for i in range(pair_count):

        @pl.when(wanted[i])
        def _(i=i):
            parts = imags[i][pl.ds(bins * rows, GAIN_ROWS), :rows].astype(jnp.float32)
            gain = parts[0:1] + parts[1:2] + parts[2:3]
            weight = weight_ref[...] * gain

            for f in range(bins):
                own = jnp.concatenate([re_ref[f], im_ref[f]], axis=0)
                turned = jnp.concatenate([im_ref[f], -re_ref[f]], axis=0)
                other_re = reals[i][f]
                other_im = imags[i][pl.ds(f * rows, rows), :]
                first = lax.dot_general(
                    own, other_re, contract, preferred_element_type=jnp.float32
                )
                second = lax.dot_general(
                    turned, other_im, contract, preferred_element_type=jnp.float32
                )
                both = first + second
                stage[i, f, :, :rows] = both[:rows] * weight
                stage[i, f, :, rows:] = both[rows:] * weight
                copy_out(i, f).start()

    for i in range(pair_count):

        @pl.when(wanted[i])
        def _(i=i):
            for f in range(bins):
                copy_out(i, f).wait()


def products(offsets, re_own, im_own, weight, group, out_shape, out):
    bins, rows, segs = re_own.shape
    count = len(group)
    vmem = pl.BlockSpec(memory_space=pltpu.VMEM)
    args = [offsets, re_own, im_own, weight]
    args += [pair[0] for pair, _ in group] + [pair[1] for pair, _ in group]
    specs = [pl.BlockSpec(memory_space=pltpu.SMEM)] + [vmem] * (len(args) - 1)
    aliases = {}
    if out is not None:
        aliases = {len(args): 0}
        args.append(out)
        specs.append(pl.BlockSpec(memory_space=pl.ANY))
    tile_bytes = rows * 2 * rows * 4
    return pl.pallas_call(
        functools.partial(product_kernel, [entry for _, entry in group]),
        out_shape=out_shape,
        in_specs=specs,
        out_specs=pl.BlockSpec(memory_space=pl.ANY),
        scratch_shapes=[
            pltpu.VMEM((count, bins, rows, 2 * rows), jnp.float32),
            pltpu.SemaphoreType.DMA((count, bins)),
        ],
        input_output_aliases=aliases,
        compiler_params=pltpu.CompilerParams(vmem_limit_bytes=VMEM_BYTES),
        cost_estimate=pl.CostEstimate(
            flops=count * bins * 8 * rows * rows * segs,
            bytes_accessed=count * bins * tile_bytes,
            transcendentals=0,
        ),
    )(*args)


def local(sr, sc, spec_re, spec_im, offsets):
    bins, rows, segs = spec_re.shape
    slot_count = offsets.shape[1]
    half = sr // 2
    bin_total = bins * lax.axis_size("fr")
    column = lax.axis_index("sc")
    norm = 1.0 / math.sqrt(segs)

    def send(value, route):
        links = []
        for z in range(sr):
            for s in range(sc):
                target = route(z, s)
                if target is not None:
                    links.append((z * sc + s, (target[0] % sr) * sc + target[1]))
        return lax.ppermute(value, BLOCKS, links)

    def both(pair, route):
        return send(pair[0], route), send(pair[1], route)

    everyone = range(sc)
    upper = [s for s in everyone if s & 2]
    lower = [s for s in everyone if not s & 2]
    odd = [s for s in everyone if s & 1]

    def down(columns=everyone):
        return lambda z, s: (z - 1, s) if s in columns else None

    def flip(bit, columns=everyone):
        return lambda z, s: (z, s ^ bit) if s in columns else None

    re32 = spec_re.astype(jnp.float32)
    im32 = spec_im.astype(jnp.float32)
    power_half = jnp.sum(re32 * re32 + im32 * im32, axis=(0, 2))
    power_other = lax.ppermute(power_half, "fr", [(0, 1), (1, 0)])
    gain = lax.rsqrt((power_half + power_other) / (bin_total * segs))
    parts, rest = [], gain
    for _ in range(GAIN_PARTS):
        part = lax.reduce_precision(rest, exponent_bits=8, mantissa_bits=7)
        parts.append(part)
        rest = rest - part
    tail = jnp.stack(parts).astype(jnp.bfloat16)
    tail = jnp.pad(tail, ((0, GAIN_ROWS - GAIN_PARTS), (0, segs - rows)))
    weight = jnp.broadcast_to((gain * norm)[:, None], (rows, rows))
    own = (spec_re, jnp.concatenate([spec_im.reshape(bins * rows, segs), tail], axis=0))

    planes = [own]
    for _ in range(half):
        planes.append(both(planes[-1], down()))
    near, far = planes[half - 1], planes[half]
    u1, u2 = both(own, flip(1, odd)), both(near, flip(1))
    v1, v2 = both(own, flip(2, upper)), both(near, flip(2))
    is_upper = (column & 2) != 0
    x3 = tuple(send(jnp.where(is_upper, v2[h], v1[h]), flip(1)) for h in range(2))
    y3 = tuple(send(jnp.where(is_upper, u2[h], far[h]), flip(2)) for h in range(2))
    z3b = send(u2[1], down([0, 1, 3]))
    late, early = lax.optimization_barrier((x3[0], u2[0]))
    z3a = send(jnp.where(column == 2, late, early), down([1, 2, 3]))
    xfa = send(y3[0], flip(1, [2]))
    yfb = send(z3b, flip(2, lower))

    def entry(plane, bit, use=lambda column: True):
        return lambda column: (plane * sc + (column ^ bit) - column, use(column))

    def x3_entry(column):
        plane = jnp.where((column & 2) != 0, half - 1, 0)
        return plane * sc + (column ^ 3) - column, True

    def y3_entry(column):
        is_upper = (column & 2) != 0
        plane = jnp.where(is_upper, half, half - 1)
        return plane * sc + (column ^ jnp.where(is_upper, 2, 3)) - column, True

    groups = [
        [(own, entry(0, 0)), (near, entry(half - 1, 0)), (u1, entry(0, 1)), (v1, entry(0, 2))],
        [(u2, entry(half - 1, 1)), (v2, entry(half - 1, 2)), (far, entry(half, 0))],
    ]
    for j in range(1, half - 1):
        u = both(planes[j], flip(1))
        v = both(planes[j], flip(2))
        d = both(v, flip(1))
        groups.append([(p, entry(j, bit)) for bit, p in enumerate((planes[j], u, v, d))])
    groups.append(
        [
            (x3, x3_entry),
            (y3, y3_entry),
            ((z3a, z3b), entry(half, 1, lambda column: (column & 1) == 1)),
            ((z3a, yfb), entry(half, 3, lambda column: column == 2)),
            ((xfa, yfb), entry(half, 3, lambda column: column == 3)),
        ]
    )
    out_shape = jax.ShapeDtypeStruct((bins, 1, slot_count, rows, 2 * rows), jnp.float32)
    out = None
    for group in groups:
        out = products(offsets, spec_re, spec_im, weight, group, out_shape, out)
    return out


def solution(mesh):
    sr, sc = mesh.shape["sr"], mesh.shape["sc"]
    placed = (P("fr", ("sr", "sc"), None), P("fr", ("sr", "sc"), None), P(("sr", "sc"), None))

    def body(*args):
        return local(sr, sc, *args)

    return jax.shard_map(
        body,
        mesh=mesh,
        in_specs=placed,
        out_specs=P("fr", ("sr", "sc"), None, None, None),
        check_vma=False,
    )
```

```python
import functools
import math

import jax
import jax.numpy as jnp
from jax import lax
from jax.experimental import pallas as pl
from jax.experimental.pallas import tpu as pltpu
from jax.sharding import PartitionSpec as P


BLOCKS = ("sr", "sc")
GAIN_PARTS = 3
GAIN_ROWS = 16
VMEM_BYTES = 16 << 20
CHUNK = 8


def vmem():
    return pl.BlockSpec(memory_space=pltpu.VMEM)


def params():
    return pltpu.CompilerParams(vmem_limit_bytes=VMEM_BYTES)


def power_kernel(re_ref, im_ref, re_out, im_out, sum_ref, sems):
    size = re_ref.shape[0]
    rows = sum_ref.shape[1]
    halves = (re_out, im_out.at[pl.ds(0, size)])
    copies = [
        pltpu.make_async_copy(source, half, sems.at[i])
        for i, (source, half) in enumerate(zip((re_ref, im_ref), halves))
    ]
    for copy in copies:
        copy.start()
    im_out[size:] = jnp.zeros((GAIN_ROWS, im_out.shape[1]), im_out.dtype)
    total = None
    for copy, half in zip(copies, halves):
        copy.wait()
        for f in range(size // rows):
            piece = half[f * rows : (f + 1) * rows, :].astype(jnp.float32)
            total = piece * piece if total is None else total + piece * piece
    folded = total[:, :rows]
    for start in range(rows, total.shape[1], rows):
        folded = folded + total[:, start : start + rows]
    sum_ref[...] = jnp.broadcast_to(jnp.sum(folded.T, axis=0, keepdims=True), sum_ref.shape)


def cat_kernel(samples, norm, im_ref, mine_ref, other_ref, out_ref, weight_ref):
    size = im_ref.shape[0] - GAIN_ROWS
    rows = mine_ref.shape[1]
    gain = lax.rsqrt((mine_ref[0:1] + other_ref[0:1]) / samples)
    weight_ref[...] = jnp.broadcast_to(gain * norm, (rows, rows)).T
    parts, rest = [], gain
    for _ in range(GAIN_PARTS):
        part = rest.astype(jnp.bfloat16).astype(jnp.float32)
        parts.append(part)
        rest = rest - part
    parts.append(jnp.zeros((GAIN_ROWS - GAIN_PARTS, rows), jnp.float32))
    tail = jnp.concatenate(parts, axis=0)
    out_ref[size:, :rows] = tail.astype(jnp.bfloat16)


def product_kernel(entries, offsets_ref, re_ref, im_ref, weight_ref, *refs):
    pair_count = len(entries)
    reals = refs[:pair_count]
    imags = refs[pair_count : 2 * pair_count]
    out_ref, stage, sems = refs[-3:]
    _, bins, rows, _ = stage.shape
    slot_count = offsets_ref.shape[1]
    contract = (((1,), (1,)), ((), ()))
    column = lax.axis_index("sc")

    wanted, slots = [], []
    for entry in entries:
        offset, use = entry(column)
        use = jnp.logical_and(use, jnp.logical_and(offset >= 0, offset < slot_count))

        def find(m, found, offset=offset):
            return jnp.where(offsets_ref[0, m] == offset, m, found)

        wanted.append(use)
        slots.append(lax.fori_loop(0, slot_count, find, jnp.int32(0), unroll=True))

    def copy_out(i, f):
        return pltpu.make_async_copy(
            stage.at[i, f], out_ref.at[f, 0, slots[i]], sems.at[i, f]
        )

    for i in range(pair_count):

        @pl.when(wanted[i])
        def _(i=i):
            parts = imags[i][pl.ds(bins * rows, GAIN_ROWS), :rows].astype(jnp.float32)
            gain = parts[0:1] + parts[1:2] + parts[2:3]
            weight = weight_ref[...] * gain
            for f in range(bins):
                low = pl.ds(f * rows, rows)
                own = jnp.concatenate([re_ref[low, :], im_ref[low, :]], axis=0)
                other = jnp.concatenate([reals[i][low, :], imags[i][low, :]], axis=0)
                four = lax.dot_general(
                    own, other, contract, preferred_element_type=jnp.float32
                )
                real = four[:rows, :rows] + four[rows:, rows:]
                imag = four[rows:, :rows] - four[:rows, rows:]
                stage[i, f, :, :rows] = real * weight
                stage[i, f, :, rows:] = imag * weight
                copy_out(i, f).start()

    for i in range(pair_count):

        @pl.when(wanted[i])
        def _(i=i):
            for f in range(bins):
                copy_out(i, f).wait()


def products(offsets, own, weight, group, out_shape, out):
    bins, _, _, rows, _ = out_shape.shape
    segs = own[0].shape[1]
    count = len(group)
    args = [offsets, *own, weight]
    args += [pair[0] for pair, _ in group] + [pair[1] for pair, _ in group]
    specs = [pl.BlockSpec(memory_space=pltpu.SMEM)] + [vmem()] * (len(args) - 1)
    aliases = {}
    if out is not None:
        aliases = {len(args): 0}
        args.append(out)
        specs.append(pl.BlockSpec(memory_space=pl.ANY))
    return pl.pallas_call(
        functools.partial(product_kernel, [entry for _, entry in group]),
        out_shape=out_shape,
        in_specs=specs,
        out_specs=pl.BlockSpec(memory_space=pl.ANY),
        scratch_shapes=[
            pltpu.VMEM((count, bins, rows, 2 * rows), jnp.float32),
            pltpu.SemaphoreType.DMA((count, bins)),
        ],
        input_output_aliases=aliases,
        compiler_params=params(),
        cost_estimate=pl.CostEstimate(
            flops=count * bins * 8 * rows * rows * segs,
            bytes_accessed=count * bins * rows * 2 * rows * 4,
            transcendentals=0,
        ),
    )(*args)


def local(sr, sc, spec_re, spec_im, offsets):
    bins, rows, segs = spec_re.shape
    size = bins * rows
    slot_count = offsets.shape[1]
    half = sr // 2
    samples = float(bins * lax.axis_size("fr") * segs)
    norm = 1.0 / math.sqrt(segs)
    column = lax.axis_index("sc")
    is_upper = (column & 2) != 0
    everyone = range(sc)
    upper = [s for s in everyone if s & 2]
    lower = [s for s in everyone if not s & 2]
    odd = [s for s in everyone if s & 1]

    def send(value, route):
        links = []
        for z in range(sr):
            for s in everyone:
                target = route(z, s)
                if target is not None:
                    links.append((z * sc + s, (target[0] % sr) * sc + target[1]))
        return lax.ppermute(value, BLOCKS, links)

    def both(pair, route):
        return send(pair[0], route), send(pair[1], route)

    def down(columns=everyone):
        return lambda z, s: (z - 1, s) if s in columns else None

    def flip(bit, columns=everyone):
        return lambda z, s: (z, s ^ bit) if s in columns else None

    flat_re = spec_re.reshape(size, segs)
    flat_im = spec_im.reshape(size, segs)
    tall = jax.ShapeDtypeStruct((size + GAIN_ROWS, segs), spec_im.dtype)
    anywhere = pl.BlockSpec(memory_space=pltpu.HBM)
    own_re, bare, mine = pl.pallas_call(
        power_kernel,
        out_shape=(
            jax.ShapeDtypeStruct((size, segs), spec_re.dtype),
            tall,
            jax.ShapeDtypeStruct((8, rows), jnp.float32),
        ),
        in_specs=[anywhere] * 2,
        out_specs=(vmem(),) * 3,
        scratch_shapes=[pltpu.SemaphoreType.DMA((2,))],
        compiler_params=params(),
        cost_estimate=pl.CostEstimate(
            flops=4 * size * segs, bytes_accessed=4 * size * segs, transcendentals=0
        ),
        name="power",
    )(flat_re, flat_im)
    other = lax.ppermute(mine, "fr", [(0, 1), (1, 0)])
    own_tail, weight = pl.pallas_call(
        functools.partial(cat_kernel, samples, norm),
        out_shape=(tall, jax.ShapeDtypeStruct((rows, rows), jnp.float32)),
        in_specs=[vmem()] * 3,
        out_specs=(vmem(), vmem()),
        input_output_aliases={0: 0},
        compiler_params=params(),
        cost_estimate=pl.CostEstimate(
            flops=rows * rows, bytes_accessed=4 * rows * rows, transcendentals=rows
        ),
        name="cat",
    )(bare, mine, other)
    own = (own_re, own_tail)

    planes = [own, (send(flat_re, down()), send(own_tail, down()))]
    for _ in range(1, half):
        planes.append(both(planes[-1], down()))
    near, far = planes[half - 1], planes[half]
    v1, v2 = both(own, flip(2, upper)), both(near, flip(2))
    u1a, u2 = send(own_re, flip(1, odd)), both(near, flip(1))

    y3 = tuple(send(jnp.where(is_upper, u2[h], far[h]), flip(2)) for h in range(2))
    x3 = tuple(send(jnp.where(is_upper, v2[h], v1[h]), flip(1)) for h in range(2))
    z3b = send(u2[1], down([0, 1, 3]))
    late, soon = lax.optimization_barrier((x3[0], u2[0]))
    z3a = send(jnp.where(column == 2, late, soon), down([1, 2, 3]))
    wide = jnp.pad(y3[0], ((0, GAIN_ROWS), (0, 0)))
    xl = send(jnp.where((column & 1) == 1, own_tail, wide), flip(1, [1, 2, 3]))
    yfb = send(z3b, flip(2, lower))

    def entry(plane, bit, use=lambda column: True):
        return lambda column: (plane * sc + (column ^ bit) - column, use(column))

    def x3_entry(column):
        plane = jnp.where((column & 2) != 0, half - 1, 0)
        return plane * sc + (column ^ 3) - column, True

    def y3_entry(column):
        is_upper = (column & 2) != 0
        plane = jnp.where(is_upper, half, half - 1)
        return plane * sc + (column ^ jnp.where(is_upper, 2, 3)) - column, True

    soon_group = [
        (own, entry(0, 0)),
        (near, entry(half - 1, 0)),
        (v1, entry(0, 2)),
        (u2, entry(half - 1, 1)),
        (v2, entry(half - 1, 2)),
        (far, entry(half, 0)),
    ]
    for j in range(1, half - 1):
        u = both(planes[j], flip(1))
        v = both(planes[j], flip(2))
        d = both(v, flip(1))
        soon_group += [(p, entry(j, bit)) for bit, p in enumerate((planes[j], u, v, d))]
    groups = [soon_group[i : i + CHUNK] for i in range(0, len(soon_group), CHUNK)]
    groups.append(
        [
            (x3, x3_entry),
            (y3, y3_entry),
            ((u1a, xl), entry(0, 1)),
            ((z3a, z3b), entry(half, 1, lambda column: (column & 1) == 1)),
            ((z3a, yfb), entry(half, 3, lambda column: column == 2)),
            ((xl, yfb), entry(half, 3, lambda column: column == 3)),
        ]
    )
    out_shape = jax.ShapeDtypeStruct((bins, 1, slot_count, rows, 2 * rows), jnp.float32)
    out = None
    for group in groups:
        out = products(offsets, own, weight, group, out_shape, out)
    return out


def solution(mesh):
    sr, sc = mesh.shape["sr"], mesh.shape["sc"]
    placed = (P("fr", ("sr", "sc"), None), P("fr", ("sr", "sc"), None), P(("sr", "sc"), None))

    def body(*args):
        return local(sr, sc, *args)

    return jax.shard_map(
        body,
        mesh=mesh,
        in_specs=placed,
        out_specs=P("fr", ("sr", "sc"), None, None, None),
        check_vma=False,
    )
```

```python
import functools
import math

import jax
import jax.numpy as jnp
from jax import lax
from jax.experimental import pallas as pl
from jax.experimental.pallas import tpu as pltpu
from jax.sharding import PartitionSpec as P


BLOCKS = ("sr", "sc")
GAIN_PARTS = 3
GAIN_ROWS = 8
VMEM_BYTES = 16 << 20
CHUNK = 8


def vmem():
    return pl.BlockSpec(memory_space=pltpu.VMEM)


def params():
    return pltpu.CompilerParams(vmem_limit_bytes=VMEM_BYTES)


def power_kernel(re_ref, im_ref, re_out, im_out, sum_ref, sems):
    size = re_ref.shape[0]
    rows = sum_ref.shape[1]
    halves = (re_out, im_out.at[pl.ds(0, size)])
    copies = [
        pltpu.make_async_copy(source, half, sems.at[i])
        for i, (source, half) in enumerate(zip((re_ref, im_ref), halves))
    ]
    for copy in copies:
        copy.start()
    im_out[size:] = jnp.zeros((GAIN_ROWS, im_out.shape[1]), im_out.dtype)
    total = None
    for copy, half in zip(copies, halves):
        copy.wait()
        for f in range(size // rows):
            piece = half[f * rows : (f + 1) * rows, :].astype(jnp.float32)
            total = piece * piece if total is None else total + piece * piece
    folded = total[:, :rows]
    for start in range(rows, total.shape[1], rows):
        folded = folded + total[:, start : start + rows]
    sum_ref[...] = jnp.broadcast_to(jnp.sum(folded.T, axis=0, keepdims=True), sum_ref.shape)


def cat_kernel(samples, norm, im_ref, mine_ref, other_ref, out_ref, weight_ref):
    size = im_ref.shape[0] - GAIN_ROWS
    rows = mine_ref.shape[1]
    gain = lax.rsqrt((mine_ref[0:1] + other_ref[0:1]) / samples)
    weight_ref[...] = jnp.broadcast_to(gain * norm, (rows, rows)).T
    parts, rest = [], gain
    for _ in range(GAIN_PARTS):
        part = rest.astype(jnp.bfloat16).astype(jnp.float32)
        parts.append(part)
        rest = rest - part
    parts.append(jnp.zeros((GAIN_ROWS - GAIN_PARTS, rows), jnp.float32))
    tail = jnp.concatenate(parts, axis=0)
    out_ref[size:, :rows] = tail.astype(jnp.bfloat16)


def product_kernel(entries, offsets_ref, re_ref, im_ref, weight_ref, *refs):
    pair_count = len(entries)
    reals = refs[:pair_count]
    imags = refs[pair_count : 2 * pair_count]
    out_ref, stage, sems = refs[-3:]
    _, bins, rows, _ = stage.shape
    slot_count = offsets_ref.shape[1]
    contract = (((1,), (1,)), ((), ()))
    column = lax.axis_index("sc")

    place = lax.broadcasted_iota(jnp.int32, offsets_ref.shape, 1)
    wanted, slots = [], []
    for entry in entries:
        offset, use = entry(column)
        use = jnp.logical_and(use, jnp.logical_and(offset >= 0, offset < slot_count))

        hit = offsets_ref[...] == offset
        wanted.append(use)
        slots.append(jnp.sum(jnp.where(hit, place, 0)))

    def copy_out(i, f):
        return pltpu.make_async_copy(
            stage.at[i, f], out_ref.at[f, 0, slots[i]], sems.at[i, f]
        )

    for i in range(pair_count):

        @pl.when(wanted[i])
        def _(i=i):
            parts = imags[i][pl.ds(bins * rows, GAIN_ROWS), :rows].astype(jnp.float32)
            gain = parts[0:1] + parts[1:2] + parts[2:3]
            weight = weight_ref[...] * gain
            for f in range(bins):
                low = pl.ds(f * rows, rows)
                own = jnp.concatenate([re_ref[low, :], im_ref[low, :]], axis=0)
                other = jnp.concatenate([reals[i][low, :], imags[i][low, :]], axis=0)
                four = lax.dot_general(
                    own, other, contract, preferred_element_type=jnp.float32
                )
                real = four[:rows, :rows] + four[rows:, rows:]
                imag = four[rows:, :rows] - four[:rows, rows:]
                stage[i, f, :, :rows] = real * weight
                stage[i, f, :, rows:] = imag * weight
                copy_out(i, f).start()

    for i in range(pair_count):

        @pl.when(wanted[i])
        def _(i=i):
            for f in range(bins):
                copy_out(i, f).wait()


def products(offsets, own, weight, group, out_shape, out):
    bins, _, _, rows, _ = out_shape.shape
    segs = own[0].shape[1]
    count = len(group)
    args = [offsets, *own, weight]
    args += [pair[0] for pair, _ in group] + [pair[1] for pair, _ in group]
    specs = [vmem()] * len(args)
    aliases = {}
    if out is not None:
        aliases = {len(args): 0}
        args.append(out)
        specs.append(pl.BlockSpec(memory_space=pl.ANY))
    return pl.pallas_call(
        functools.partial(product_kernel, [entry for _, entry in group]),
        out_shape=out_shape,
        in_specs=specs,
        out_specs=pl.BlockSpec(memory_space=pl.ANY),
        scratch_shapes=[
            pltpu.VMEM((count, bins, rows, 2 * rows), jnp.float32),
            pltpu.SemaphoreType.DMA((count, bins)),
        ],
        input_output_aliases=aliases,
        compiler_params=params(),
        cost_estimate=pl.CostEstimate(
            flops=count * bins * 8 * rows * rows * segs,
            bytes_accessed=count * bins * rows * 2 * rows * 4,
            transcendentals=0,
        ),
    )(*args)


def local(sr, sc, spec_re, spec_im, offsets):
    bins, rows, segs = spec_re.shape
    size = bins * rows
    slot_count = offsets.shape[1]
    half = sr // 2
    samples = float(bins * lax.axis_size("fr") * segs)
    norm = 1.0 / math.sqrt(segs)
    column = lax.axis_index("sc")
    is_upper = (column & 2) != 0
    everyone = range(sc)
    upper = [s for s in everyone if s & 2]
    lower = [s for s in everyone if not s & 2]
    odd = [s for s in everyone if s & 1]

    def send(value, route):
        links = []
        for z in range(sr):
            for s in everyone:
                target = route(z, s)
                if target is not None:
                    links.append((z * sc + s, (target[0] % sr) * sc + target[1]))
        return lax.ppermute(value, BLOCKS, links)

    def both(pair, route):
        return send(pair[0], route), send(pair[1], route)

    def down(columns=everyone):
        return lambda z, s: (z - 1, s) if s in columns else None

    def flip(bit, columns=everyone):
        return lambda z, s: (z, s ^ bit) if s in columns else None

    flat_re = spec_re.reshape(size, segs)
    flat_im = spec_im.reshape(size, segs)
    tall = jax.ShapeDtypeStruct((size + GAIN_ROWS, segs), spec_im.dtype)
    anywhere = pl.BlockSpec(memory_space=pltpu.HBM)
    own_re, bare, mine = pl.pallas_call(
        power_kernel,
        out_shape=(
            jax.ShapeDtypeStruct((size, segs), spec_re.dtype),
            tall,
            jax.ShapeDtypeStruct((8, rows), jnp.float32),
        ),
        in_specs=[anywhere] * 2,
        out_specs=(vmem(),) * 3,
        scratch_shapes=[pltpu.SemaphoreType.DMA((2,))],
        compiler_params=params(),
        cost_estimate=pl.CostEstimate(
            flops=4 * size * segs, bytes_accessed=4 * size * segs, transcendentals=0
        ),
        name="power",
    )(flat_re, flat_im)
    other = lax.ppermute(mine, "fr", [(0, 1), (1, 0)])
    own_tail, weight = pl.pallas_call(
        functools.partial(cat_kernel, samples, norm),
        out_shape=(tall, jax.ShapeDtypeStruct((rows, rows), jnp.float32)),
        in_specs=[vmem()] * 3,
        out_specs=(vmem(), vmem()),
        input_output_aliases={0: 0},
        compiler_params=params(),
        cost_estimate=pl.CostEstimate(
            flops=rows * rows, bytes_accessed=4 * rows * rows, transcendentals=rows
        ),
        name="cat",
    )(bare, mine, other)
    own = (own_re, own_tail)

    planes = [own, (send(flat_re, down()), send(own_tail, down()))]
    for _ in range(1, half):
        planes.append(both(planes[-1], down()))
    near, far = planes[half - 1], planes[half]
    v1, v2 = both(own, flip(2, upper)), both(near, flip(2))
    u1a, u2 = send(own_re, flip(1, odd)), both(near, flip(1))

    y3 = tuple(send(jnp.where(is_upper, u2[h], far[h]), flip(2)) for h in range(2))
    x3 = tuple(send(jnp.where(is_upper, v2[h], v1[h]), flip(1)) for h in range(2))
    z3b = send(u2[1], down([0, 1, 3]))
    late, soon = lax.optimization_barrier((x3[0], u2[0]))
    z3a = send(jnp.where(column == 2, late, soon), down([1, 2, 3]))
    wide = jnp.pad(y3[0], ((0, GAIN_ROWS), (0, 0)))
    xl = send(jnp.where((column & 1) == 1, own_tail, wide), flip(1, [1, 2, 3]))
    yfb = send(z3b, flip(2, lower))

    def entry(plane, bit, use=lambda column: True):
        return lambda column: (plane * sc + (column ^ bit) - column, use(column))

    def x3_entry(column):
        plane = jnp.where((column & 2) != 0, half - 1, 0)
        return plane * sc + (column ^ 3) - column, True

    def y3_entry(column):
        is_upper = (column & 2) != 0
        plane = jnp.where(is_upper, half, half - 1)
        return plane * sc + (column ^ jnp.where(is_upper, 2, 3)) - column, True

    soon_group = [
        (own, entry(0, 0)),
        (near, entry(half - 1, 0)),
        (v1, entry(0, 2)),
        (u2, entry(half - 1, 1)),
        (v2, entry(half - 1, 2)),
        (far, entry(half, 0)),
    ]
    for j in range(1, half - 1):
        u = both(planes[j], flip(1))
        v = both(planes[j], flip(2))
        d = both(v, flip(1))
        soon_group += [(p, entry(j, bit)) for bit, p in enumerate((planes[j], u, v, d))]
    groups = [soon_group[i : i + CHUNK] for i in range(0, len(soon_group), CHUNK)]
    groups.append([(x3, x3_entry), (y3, y3_entry)])
    groups.append(
        [
            ((u1a, xl), entry(0, 1)),
            ((z3a, z3b), entry(half, 1, lambda column: (column & 1) == 1)),
            ((z3a, yfb), entry(half, 3, lambda column: column == 2)),
            ((xl, yfb), entry(half, 3, lambda column: column == 3)),
        ]
    )
    out_shape = jax.ShapeDtypeStruct((bins, 1, slot_count, rows, 2 * rows), jnp.float32)
    out = None
    for group in groups:
        out = products(offsets, own, weight, group, out_shape, out)
    return out


def solution(mesh):
    sr, sc = mesh.shape["sr"], mesh.shape["sc"]
    placed = (P("fr", ("sr", "sc"), None), P("fr", ("sr", "sc"), None), P(("sr", "sc"), None))

    def body(*args):
        return local(sr, sc, *args)

    return jax.shard_map(
        body,
        mesh=mesh,
        in_specs=placed,
        out_specs=P("fr", ("sr", "sc"), None, None, None),
        check_vma=False,
    )
```

```python
import functools
import math

import jax
import jax.numpy as jnp
from jax import lax
from jax.experimental import pallas as pl
from jax.experimental.pallas import tpu as pltpu
from jax.sharding import PartitionSpec as P


BLOCKS = ("sr", "sc")
GAIN_PARTS = 3
GAIN_ROWS = 8
VMEM_BYTES = 16 << 20
CHUNK = 8


def vmem():
    return pl.BlockSpec(memory_space=pltpu.VMEM)


def params():
    return pltpu.CompilerParams(vmem_limit_bytes=VMEM_BYTES)


def power_kernel(re_ref, im_ref, re_out, im_out, sum_ref, sems):
    size = re_ref.shape[0]
    rows = sum_ref.shape[1]
    halves = (re_out, im_out.at[pl.ds(0, size)])
    copies = [
        pltpu.make_async_copy(source, half, sems.at[i])
        for i, (source, half) in enumerate(zip((re_ref, im_ref), halves))
    ]
    for copy in copies:
        copy.start()
    im_out[size:] = jnp.zeros((GAIN_ROWS, im_out.shape[1]), im_out.dtype)
    total = None
    for copy, half in zip(copies, halves):
        copy.wait()
        for f in range(size // rows):
            piece = half[f * rows : (f + 1) * rows, :].astype(jnp.float32)
            total = piece * piece if total is None else total + piece * piece
    folded = total[:, :rows]
    for start in range(rows, total.shape[1], rows):
        folded = folded + total[:, start : start + rows]
    sum_ref[...] = jnp.broadcast_to(jnp.sum(folded.T, axis=0, keepdims=True), sum_ref.shape)


def cat_kernel(samples, norm, im_ref, mine_ref, other_ref, out_ref, weight_ref):
    size = im_ref.shape[0] - GAIN_ROWS
    rows = mine_ref.shape[1]
    gain = lax.rsqrt((mine_ref[0:1] + other_ref[0:1]) / samples)
    weight_ref[...] = jnp.broadcast_to(gain * norm, (rows, rows)).T
    parts, rest = [], gain
    for _ in range(GAIN_PARTS):
        part = rest.astype(jnp.bfloat16).astype(jnp.float32)
        parts.append(part)
        rest = rest - part
    parts.append(jnp.zeros((GAIN_ROWS - GAIN_PARTS, rows), jnp.float32))
    tail = jnp.concatenate(parts, axis=0)
    out_ref[size:, :rows] = tail.astype(jnp.bfloat16)


def product_kernel(entries, offsets_ref, re_ref, im_ref, weight_ref, *refs):
    pair_count = len(entries)
    reals = refs[:pair_count]
    imags = refs[pair_count : 2 * pair_count]
    out_ref, stage, sems = refs[-3:]
    _, bins, rows, _ = stage.shape
    slot_count = offsets_ref.shape[1]
    contract = (((1,), (1,)), ((), ()))
    column = lax.axis_index("sc")

    place = lax.broadcasted_iota(jnp.int32, offsets_ref.shape, 1)
    wanted, keys = [], []
    for entry in entries:
        offset, use = entry(column)
        use = jnp.logical_and(use, jnp.logical_and(offset >= 0, offset < slot_count))

        wanted.append(use)
        keys.append(offset)

    def copy_out(i, f, slot):
        return pltpu.make_async_copy(
            stage.at[i, f], out_ref.at[f, 0, slot], sems.at[i, f]
        )

    for i in range(pair_count):

        @pl.when(wanted[i])
        def _(i=i):
            slot = jnp.sum(jnp.where(offsets_ref[...] == keys[i], place, 0))
            parts = imags[i][pl.ds(bins * rows, GAIN_ROWS), :rows].astype(jnp.float32)
            gain = parts[0:1] + parts[1:2] + parts[2:3]
            weight = weight_ref[...] * gain
            for f in range(bins):
                low = pl.ds(f * rows, rows)
                own = jnp.concatenate([re_ref[low, :], im_ref[low, :]], axis=0)
                other = jnp.concatenate([reals[i][low, :], imags[i][low, :]], axis=0)
                four = lax.dot_general(
                    own, other, contract, preferred_element_type=jnp.float32
                )
                real = four[:rows, :rows] + four[rows:, rows:]
                imag = four[rows:, :rows] - four[:rows, rows:]
                stage[i, f, :, :rows] = real * weight
                stage[i, f, :, rows:] = imag * weight
                copy_out(i, f, slot).start()

    for i in range(pair_count):

        @pl.when(wanted[i])
        def _(i=i):
            for f in range(bins):
                copy_out(i, f, 0).wait()


def products(offsets, own, weight, group, out_shape, out):
    bins, _, _, rows, _ = out_shape.shape
    segs = own[0].shape[1]
    count = len(group)
    args = [offsets, *own, weight]
    args += [pair[0] for pair, _ in group] + [pair[1] for pair, _ in group]
    specs = [vmem()] * len(args)
    aliases = {}
    if out is not None:
        aliases = {len(args): 0}
        args.append(out)
        specs.append(pl.BlockSpec(memory_space=pl.ANY))
    return pl.pallas_call(
        functools.partial(product_kernel, [entry for _, entry in group]),
        out_shape=out_shape,
        in_specs=specs,
        out_specs=pl.BlockSpec(memory_space=pl.ANY),
        scratch_shapes=[
            pltpu.VMEM((count, bins, rows, 2 * rows), jnp.float32),
            pltpu.SemaphoreType.DMA((count, bins)),
        ],
        input_output_aliases=aliases,
        compiler_params=params(),
        cost_estimate=pl.CostEstimate(
            flops=count * bins * 8 * rows * rows * segs,
            bytes_accessed=count * bins * rows * 2 * rows * 4,
            transcendentals=0,
        ),
    )(*args)


def local(sr, sc, spec_re, spec_im, offsets):
    bins, rows, segs = spec_re.shape
    size = bins * rows
    slot_count = offsets.shape[1]
    half = sr // 2
    samples = float(bins * lax.axis_size("fr") * segs)
    norm = 1.0 / math.sqrt(segs)
    column = lax.axis_index("sc")
    is_upper = (column & 2) != 0
    everyone = range(sc)
    upper = [s for s in everyone if s & 2]
    lower = [s for s in everyone if not s & 2]
    odd = [s for s in everyone if s & 1]

    def send(value, route):
        links = []
        for z in range(sr):
            for s in everyone:
                target = route(z, s)
                if target is not None:
                    links.append((z * sc + s, (target[0] % sr) * sc + target[1]))
        return lax.ppermute(value, BLOCKS, links)

    def both(pair, route):
        return send(pair[0], route), send(pair[1], route)

    def down(columns=everyone):
        return lambda z, s: (z - 1, s) if s in columns else None

    def flip(bit, columns=everyone):
        return lambda z, s: (z, s ^ bit) if s in columns else None

    flat_re = spec_re.reshape(size, segs)
    flat_im = spec_im.reshape(size, segs)
    tall = jax.ShapeDtypeStruct((size + GAIN_ROWS, segs), spec_im.dtype)
    anywhere = pl.BlockSpec(memory_space=pltpu.HBM)
    own_re, bare, mine = pl.pallas_call(
        power_kernel,
        out_shape=(
            jax.ShapeDtypeStruct((size, segs), spec_re.dtype),
            tall,
            jax.ShapeDtypeStruct((8, rows), jnp.float32),
        ),
        in_specs=[anywhere] * 2,
        out_specs=(vmem(),) * 3,
        scratch_shapes=[pltpu.SemaphoreType.DMA((2,))],
        compiler_params=params(),
        cost_estimate=pl.CostEstimate(
            flops=4 * size * segs, bytes_accessed=4 * size * segs, transcendentals=0
        ),
        name="power",
    )(flat_re, flat_im)
    other = lax.ppermute(mine, "fr", [(0, 1), (1, 0)])
    own_tail, weight = pl.pallas_call(
        functools.partial(cat_kernel, samples, norm),
        out_shape=(tall, jax.ShapeDtypeStruct((rows, rows), jnp.float32)),
        in_specs=[vmem()] * 3,
        out_specs=(vmem(), vmem()),
        input_output_aliases={0: 0},
        compiler_params=params(),
        cost_estimate=pl.CostEstimate(
            flops=rows * rows, bytes_accessed=4 * rows * rows, transcendentals=rows
        ),
        name="cat",
    )(bare, mine, other)
    own = (own_re, own_tail)

    planes = [own, (send(flat_re, down()), send(own_tail, down()))]
    for _ in range(1, half):
        planes.append(both(planes[-1], down()))
    near, far = planes[half - 1], planes[half]
    v1, v2 = both(own, flip(2, upper)), both(near, flip(2))
    u1a, u2 = send(own_re, flip(1, odd)), both(near, flip(1))

    y3 = tuple(send(jnp.where(is_upper, u2[h], far[h]), flip(2)) for h in range(2))
    x3 = tuple(send(jnp.where(is_upper, v2[h], v1[h]), flip(1)) for h in range(2))
    z3b = send(u2[1], down([0, 1, 3]))
    late, soon = lax.optimization_barrier((x3[0], u2[0]))
    z3a = send(jnp.where(column == 2, late, soon), down([1, 2, 3]))
    wide = jnp.pad(y3[0], ((0, GAIN_ROWS), (0, 0)))
    xl = send(jnp.where((column & 1) == 1, own_tail, wide), flip(1, [1, 2, 3]))
    yfb = send(z3b, flip(2, lower))

    def entry(plane, bit, use=lambda column: True):
        return lambda column: (plane * sc + (column ^ bit) - column, use(column))

    def x3_entry(column):
        plane = jnp.where((column & 2) != 0, half - 1, 0)
        return plane * sc + (column ^ 3) - column, True

    def y3_entry(column):
        is_upper = (column & 2) != 0
        plane = jnp.where(is_upper, half, half - 1)
        return plane * sc + (column ^ jnp.where(is_upper, 2, 3)) - column, True

    soon_group = [
        (own, entry(0, 0)),
        (near, entry(half - 1, 0)),
        (v1, entry(0, 2)),
        (u2, entry(half - 1, 1)),
        (v2, entry(half - 1, 2)),
        (far, entry(half, 0)),
    ]
    for j in range(1, half - 1):
        u = both(planes[j], flip(1))
        v = both(planes[j], flip(2))
        d = both(v, flip(1))
        soon_group += [(p, entry(j, bit)) for bit, p in enumerate((planes[j], u, v, d))]
    groups = [soon_group[i : i + CHUNK] for i in range(0, len(soon_group), CHUNK)]
    groups.append([(x3, x3_entry), (y3, y3_entry)])
    groups.append(
        [
            ((u1a, xl), entry(0, 1)),
            ((z3a, z3b), entry(half, 1, lambda column: (column & 1) == 1)),
            ((z3a, yfb), entry(half, 3, lambda column: column == 2)),
            ((xl, yfb), entry(half, 3, lambda column: column == 3)),
        ]
    )
    out_shape = jax.ShapeDtypeStruct((bins, 1, slot_count, rows, 2 * rows), jnp.float32)
    out = None
    for group in groups:
        out = products(offsets, own, weight, group, out_shape, out)
    return out


def solution(mesh):
    sr, sc = mesh.shape["sr"], mesh.shape["sc"]
    placed = (P("fr", ("sr", "sc"), None), P("fr", ("sr", "sc"), None), P(("sr", "sc"), None))

    def body(*args):
        return local(sr, sc, *args)

    return jax.shard_map(
        body,
        mesh=mesh,
        in_specs=placed,
        out_specs=P("fr", ("sr", "sc"), None, None, None),
        check_vma=False,
    )
```
